64 devices in a mesh: data: 4 (over x, y), seq: 16 (over z, core).
Axes of the slice: x: 2, y: 2, z: 8, core: 2. Of those that a mesh axis runs over, the one named last changes fastest.
The devices are a block of a 4x4x8 slice.
Arguments:
- x_in: bfloat16 [16, 4096, 2048], P(None, ('data', 'seq')), parts along dimension 1
- positions: int32 [4096], P(('data', 'seq')), parts along dimension 0
- w_query: bfloat16 [3, 2048, 16, 128], replicated
- w_key: bfloat16 [3, 2048, 16, 128], replicated
- w_value: bfloat16 [3, 2048, 16, 128], replicated
- w_out: bfloat16 [3, 16, 128, 2048], replicated
- w_up: bfloat16 [3, 2048, 8192], replicated
- w_down: bfloat16 [3, 8192, 2048], replicated
- g_attn: float32 [3, 2048], replicated
- g_mlp: float32 [3, 2048], replicated
Outputs:
- output: bfloat16 [16, 4096, 2048], P(None, ('data', 'seq')), parts along dimension 1
There are 4 independent parts. The reference program is written for one: setup_inputs(seed, part) draws one part's arguments, and reference() takes and returns one part's arrays. A program takes and returns all parts, laid end to end along the dimension named above; an argument that names none is the same for every part.
All inputs are finite; a program needn't handle non-finite values.
Results may differ from the reference program's by a relative error of at most 0.0163719.
Values are sent between devices in bfloat16 or wider.
A program may use at most 768 MiB of HBM per device.

```python
import jax
import jax.numpy as jnp
from jax import lax

BATCH_SIZE = 16
SEQ_LEN = 1024
D_MODEL = 2048
N_HEADS = 16
N_KV_HEADS = 16
HEAD_DIM = 128
FF_DIM = 8192
N_LAYERS = 3
REF_BLOCK = 64

ROPE_BASE = 10000.0
NORM_EPS = 1e-6


def normal_weights(rng_key, w_shape, fan_in, w_gain):
    return (jax.random.normal(rng_key, w_shape, jnp.float32) * (w_gain * fan_in ** -0.5)).astype(jnp.bfloat16)


def setup_inputs(seed: int = 0, part: int = 0) -> dict:
    base_key = jax.random.key(seed)
    part_keys = jax.random.split(jax.random.fold_in(base_key, part), 6)
    weight_keys = jax.random.split(jax.random.fold_in(base_key, 100003), 8)
    step_frac = jnp.arange(SEQ_LEN, dtype=jnp.float32) / SEQ_LEN
    wave_freq = jax.random.uniform(part_keys[0], (BATCH_SIZE, 4), jnp.float32, minval=0.5, maxval=3.0)
    wave_phase = jax.random.uniform(part_keys[1], (BATCH_SIZE, 4), jnp.float32, minval=0.0, maxval=6.283185)
    wave_vals = jnp.cos(6.283185 * wave_freq[:, :, None] * step_frac[None, None, :] + wave_phase[:, :, None])
    wave_dirs = jax.random.normal(part_keys[2], (BATCH_SIZE, 4, D_MODEL), jnp.float32)
    smooth = jnp.einsum("bjs,bjd->bsd", wave_vals, wave_dirs) * 0.5
    noise_part = jax.random.normal(part_keys[3], (BATCH_SIZE, SEQ_LEN, D_MODEL), jnp.float32) * 0.7
    offset = jax.random.randint(part_keys[4], (), 0, SEQ_LEN)
    pos_gaps = jax.random.randint(part_keys[5], (SEQ_LEN,), 1, 5)
    return {
        "x_in": (smooth + noise_part).astype(jnp.bfloat16),
        "positions": (offset + jnp.cumsum(pos_gaps)).astype(jnp.int32),
        "w_query": normal_weights(weight_keys[0], (N_LAYERS, D_MODEL, N_HEADS, HEAD_DIM), D_MODEL, 1.25),
        "w_key": normal_weights(weight_keys[1], (N_LAYERS, D_MODEL, N_KV_HEADS, HEAD_DIM), D_MODEL, 1.25),
        "w_value": normal_weights(weight_keys[2], (N_LAYERS, D_MODEL, N_KV_HEADS, HEAD_DIM), D_MODEL, 1.0),
        "w_out": normal_weights(weight_keys[3], (N_LAYERS, N_HEADS, HEAD_DIM, D_MODEL), N_HEADS * HEAD_DIM, 1.0),
        "w_up": normal_weights(weight_keys[4], (N_LAYERS, D_MODEL, FF_DIM), D_MODEL, 1.0),
        "w_down": normal_weights(weight_keys[5], (N_LAYERS, FF_DIM, D_MODEL), FF_DIM, 1.0),
        "g_attn": jax.random.uniform(weight_keys[6], (N_LAYERS, D_MODEL), jnp.float32, minval=0.5, maxval=1.5),
        "g_mlp": jax.random.uniform(weight_keys[7], (N_LAYERS, D_MODEL), jnp.float32, minval=0.5, maxval=1.5),
    }


def rms_norm(x_act, gain_vec):
    x_f32 = x_act.astype(jnp.float32)
    mean_sq = jnp.mean(x_f32 * x_f32, axis=-1, keepdims=True)
    return (x_f32 * lax.rsqrt(mean_sq + NORM_EPS) * gain_vec).astype(jnp.bfloat16)


def rope_tables(positions):
    inv_freq = ROPE_BASE ** (-jnp.arange(HEAD_DIM // 2, dtype=jnp.float32) * (2.0 / HEAD_DIM))
    angles = positions.astype(jnp.float32)[:, None] * inv_freq[None, :]
    return jnp.cos(angles), jnp.sin(angles)


def apply_rope(proj_f32, cos_t, sin_t):
    half_dim = HEAD_DIM // 2
    x_first = proj_f32[..., :half_dim]
    x_second = proj_f32[..., half_dim:]
    cos_b = cos_t[:, None, :]
    sin_b = sin_t[:, None, :]
    return jnp.concatenate([x_first * cos_b - x_second * sin_b, x_second * cos_b + x_first * sin_b], axis=-1).astype(jnp.bfloat16)


def causal_attention(q_heads, k_heads, v_heads):
    groups = N_HEADS // N_KV_HEADS
    n_blocks = SEQ_LEN // REF_BLOCK
    att_scale = HEAD_DIM ** -0.5
    q_grouped = q_heads.reshape(BATCH_SIZE, SEQ_LEN, N_KV_HEADS, groups, HEAD_DIM)
    k_f32 = k_heads.astype(jnp.float32)
    v_f32 = v_heads.astype(jnp.float32)
    key_pos = jnp.arange(SEQ_LEN)

    def one_block(blk_idx):
        blk_start = blk_idx * REF_BLOCK
        q_blk = lax.dynamic_slice_in_dim(q_grouped, blk_start, REF_BLOCK, axis=1).astype(jnp.float32)
        scores = jnp.einsum("bqkgd,bskd->bkgqs", q_blk, k_f32) * att_scale
        query_pos = blk_start + jnp.arange(REF_BLOCK)
        allowed = key_pos[None, :] <= query_pos[:, None]
        scores = jnp.where(allowed, scores, -1e30)
        row_max = jnp.max(scores, axis=-1, keepdims=True)
        exp_f32 = jnp.exp(scores - row_max)
        row_sum = jnp.sum(exp_f32, axis=-1)
        weighted = jnp.einsum("bkgqs,bskd->bqkgd", exp_f32.astype(jnp.bfloat16).astype(jnp.float32), v_f32)
        return (weighted / jnp.transpose(row_sum, (0, 3, 1, 2))[..., None]).astype(jnp.bfloat16)

    blocks = lax.map(one_block, jnp.arange(n_blocks))
    return jnp.moveaxis(blocks, 0, 1).reshape(BATCH_SIZE, SEQ_LEN, N_HEADS, HEAD_DIM)


def transformer_layer(hidden, cos_t, sin_t, layer_weights):
    w_query, w_key, w_value, w_out, w_up, w_down, gain_attn, gain_mlp = layer_weights
    n_rows = BATCH_SIZE * SEQ_LEN
    normed = rms_norm(hidden, gain_attn).reshape(n_rows, D_MODEL)
    q_proj = jnp.dot(normed, w_query.reshape(D_MODEL, N_HEADS * HEAD_DIM), preferred_element_type=jnp.float32)
    k_proj = jnp.dot(normed, w_key.reshape(D_MODEL, N_KV_HEADS * HEAD_DIM), preferred_element_type=jnp.float32)
    v_proj = jnp.dot(normed, w_value.reshape(D_MODEL, N_KV_HEADS * HEAD_DIM), preferred_element_type=jnp.float32)
    q_heads = apply_rope(q_proj.reshape(BATCH_SIZE, SEQ_LEN, N_HEADS, HEAD_DIM), cos_t, sin_t)
    k_heads = apply_rope(k_proj.reshape(BATCH_SIZE, SEQ_LEN, N_KV_HEADS, HEAD_DIM), cos_t, sin_t)
    v_heads = v_proj.astype(jnp.bfloat16).reshape(BATCH_SIZE, SEQ_LEN, N_KV_HEADS, HEAD_DIM)
    attn_out = causal_attention(q_heads, k_heads, v_heads)
    attn_proj = jnp.dot(attn_out.reshape(n_rows, N_HEADS * HEAD_DIM), w_out.reshape(N_HEADS * HEAD_DIM, D_MODEL), preferred_element_type=jnp.float32)
    resid_h = (hidden.reshape(n_rows, D_MODEL).astype(jnp.float32) + attn_proj).astype(jnp.bfloat16)
    normed_mlp = rms_norm(resid_h, gain_mlp)
    gelu_act = jax.nn.gelu(jnp.dot(normed_mlp, w_up, preferred_element_type=jnp.float32), approximate=True).astype(jnp.bfloat16)
    layer_out = resid_h.astype(jnp.float32) + jnp.dot(gelu_act, w_down, preferred_element_type=jnp.float32)
    return layer_out.astype(jnp.bfloat16).reshape(BATCH_SIZE, SEQ_LEN, D_MODEL)


def reference(x_in, positions, w_query, w_key, w_value, w_out, w_up, w_down, g_attn, g_mlp):
    cos_t, sin_t = rope_tables(positions)

    def layer_body(hidden, layer_weights):
        return transformer_layer(hidden, cos_t, sin_t, layer_weights), None

    stacked = (w_query, w_key, w_value, w_out, w_up, w_down, g_attn, g_mlp)
    return lax.scan(layer_body, x_in, stacked)[0]
```

```python
import functools
import jax
import jax.numpy as jnp
from jax import lax
from jax.experimental import pallas as pl
from jax.experimental.pallas import tpu as pltpu
from jax.sharding import PartitionSpec as P

EPS = 1e-6
F32 = jnp.float32
BF16 = jnp.bfloat16


def norm_rows(x, g):
    x = x.astype(F32)
    return (x * lax.rsqrt(jnp.mean(x * x, axis=-1, keepdims=True) + EPS) * g).astype(BF16)


def gelu(x):
    h = 0.5 * x
    return h * jnp.tanh(x * (0.7978845608028654 + 0.035677408136300125 * (x * x))) + h


def row_loop(rows, tile, body):
    if rows == tile:
        body(0)
        return
    def step(i, c):
        body(pl.multiple_of(i * tile, tile))
        return c
    lax.fori_loop(0, rows // tile, step, 0)


def qkv_kernel(nq, tm, x_ref, g_ref, cos_ref, sin_ref, wq, wk, wv, q_ref, k_ref, v_ref, n_ref):
    s = pl.program_id(0)
    rows = x_ref.shape[0]
    dh = cos_ref.shape[1]

    @pl.when(s == 0)
    def _():
        def nb(r):
            n_ref[pl.ds(r, 128), :] = norm_rows(x_ref[pl.ds(r, 128), :], g_ref[0])
        row_loop(rows, 128, nb)

    def proj(w_ref, o_ref, rope):
        def mb(r):
            u = jnp.dot(n_ref[pl.ds(r, tm), :], w_ref[0], preferred_element_type=F32)
            if not rope:
                o_ref[pl.ds(r, tm), :] = u.astype(BF16)
            else:
                c = cos_ref[pl.ds(r, tm), :]
                sn = sin_ref[pl.ds(r, tm), :]
                for h in range(u.shape[1] // dh):
                    uh = u[:, h * dh:(h + 1) * dh]
                    o_ref[pl.ds(r, tm), h * dh:(h + 1) * dh] = (uh * c + pltpu.roll(uh, dh // 2, 1) * sn).astype(BF16)
        row_loop(rows, tm, mb)

    pl.when(s < nq)(lambda: proj(wq, q_ref, True))
    pl.when((s >= nq) & (s < 2 * nq))(lambda: proj(wk, k_ref, True))
    pl.when(s >= 2 * nq)(lambda: proj(wv, v_ref, False))


def qkv_call(x, g, cos, sin, wq, wk, wv, layer, tn=512, tm=512):
    rows, d = x.shape
    hd = wq.shape[2]
    nq = hd // tn
    def wmap(i):
        return lambda s: (layer, 0, jnp.clip(s - i * nq, 0, nq - 1))
    def omap(i):
        return lambda s: (0, jnp.clip(s - i * nq, 0, nq - 1))
    full = lambda a: pl.BlockSpec(a.shape, lambda s: (0,) * a.ndim)
    out = jax.ShapeDtypeStruct((rows, hd), BF16)
    return pl.pallas_call(
        functools.partial(qkv_kernel, nq, tm),
        grid=(3 * nq,),
        in_specs=[full(x), pl.BlockSpec((1, 1, d), lambda s: (layer, 0, 0)), full(cos), full(sin)]
        + [pl.BlockSpec((1, d, tn), wmap(i)) for i in range(3)],
        out_specs=[pl.BlockSpec((rows, tn), omap(i)) for i in range(3)],
        out_shape=[out, out, out],
        scratch_shapes=[pltpu.VMEM((rows, d), BF16)],
        compiler_params=pltpu.CompilerParams(vmem_limit_bytes=56 * 2**20),
        cost_estimate=pl.CostEstimate(flops=6 * rows * d * hd, bytes_accessed=6 * d * hd, transcendentals=0),
        name="qkv",
    )(x, g, cos, sin, wq, wk, wv)


def attn_kernel(dh, tq, q_ref, k_ref, v_ref, o_ref):
    rows = q_ref.shape[0]
    scale = dh ** -0.5 * 1.4426950408889634
    r = lax.broadcasted_iota(jnp.int32, (tq, tq), 0)
    c = lax.broadcasted_iota(jnp.int32, (tq, tq), 1)
    keep = c <= r
    jobs = [(h, i) for h in range(q_ref.shape[1] // dh) for i in range(rows // tq)]
    def score(job):
        h, i = job
        cs = slice(h * dh, (h + 1) * dh)
        n = (i + 1) * tq
        return lax.dot_general(q_ref[i * tq:n, cs], k_ref[:n, cs], (((1,), (1,)), ((), ())), preferred_element_type=F32)
    nxt = score(jobs[0])
    for j, (h, i) in enumerate(jobs):
        s = nxt
        if j + 1 < len(jobs):
            nxt = score(jobs[j + 1])
        cs = slice(h * dh, (h + 1) * dh)
        n = (i + 1) * tq
        sd = jnp.where(keep, s[:, n - tq:], -1e30)
        s = jnp.concatenate([s[:, :n - tq], sd], axis=1) if i else sd
        m = jnp.max(s, axis=1, keepdims=True)
        e = jnp.exp2((s - m) * scale)
        l = jnp.sum(e, axis=1, keepdims=True)
        o = jnp.dot(e.astype(BF16), v_ref[:n, cs], preferred_element_type=F32)
        o_ref[i * tq:n, cs] = (o / l).astype(BF16)


def attn_call(q, k, v, dh=128, tq=256, hb=1):
    rows, hd = q.shape
    spec = pl.BlockSpec((rows, dh * hb), lambda h: (0, h))
    return pl.pallas_call(
        functools.partial(attn_kernel, dh, tq),
        grid=(hd // dh // hb,),
        in_specs=[spec] * 3,
        out_specs=spec,
        out_shape=jax.ShapeDtypeStruct((rows, hd), BF16),
        compiler_params=pltpu.CompilerParams(vmem_limit_bytes=56 * 2**20),
        cost_estimate=pl.CostEstimate(flops=2 * rows * rows * hd, bytes_accessed=8 * rows * hd, transcendentals=0),
        name="attn",
    )(q, k, v)


def mlp_kernel(no, nf, tm, o_ref, x_ref, g_ref, wo, wu, wd, y_ref, h_ref, r_ref, acc_ref):
    s = pl.program_id(0)
    rows, d = x_ref.shape
    tn = wo.shape[2]

    @pl.when(s < no)
    def _():
        def mb(r):
            cs = pl.ds(pl.multiple_of(s * tn, tn), tn)
            u = jnp.dot(o_ref[pl.ds(r, tm), :], wo[0], preferred_element_type=F32)
            h_ref[pl.ds(r, tm), cs] = (x_ref[pl.ds(r, tm), cs].astype(F32) + u).astype(BF16)
        row_loop(rows, tm, mb)

    @pl.when(s == no)
    def _():
        def nb(r):
            h = h_ref[pl.ds(r, 128), :]
            r_ref[pl.ds(r, 128), :] = norm_rows(h, g_ref[0])
            acc_ref[pl.ds(r, 128), :] = h.astype(F32)
        row_loop(rows, 128, nb)

    @pl.when(s >= no)
    def _():
        def mb(r):
            z = jnp.dot(r_ref[pl.ds(r, tm), :], wu[0], preferred_element_type=F32)
            z = gelu(z).astype(BF16)
            acc_ref[pl.ds(r, tm), :] += jnp.dot(z, wd[0], preferred_element_type=F32)
        row_loop(rows, tm, mb)

    @pl.when(s == no + nf - 1)
    def _():
        def nb(r):
            y_ref[pl.ds(r, 128), :] = acc_ref[pl.ds(r, 128), :].astype(BF16)
        row_loop(rows, 128, nb)


def mlp_call(o, x, g, wo, wu, wd, layer, tn=512, tf=512, tm=512):
    rows, d = x.shape
    f = wu.shape[2]
    no, nf = d // tn, f // tf
    full = lambda a: pl.BlockSpec(a.shape, lambda s: (0,) * a.ndim)
    return pl.pallas_call(
        functools.partial(mlp_kernel, no, nf, tm),
        grid=(no + nf,),
        in_specs=[full(o), full(x), pl.BlockSpec((1, 1, d), lambda s: (layer, 0, 0)),
                  pl.BlockSpec((1, wo.shape[1], tn), lambda s: (layer, 0, jnp.minimum(s, no - 1))),
                  pl.BlockSpec((1, d, tf), lambda s: (layer, 0, jnp.maximum(s - no, 0))),
                  pl.BlockSpec((1, tf, d), lambda s: (layer, jnp.maximum(s - no, 0), 0))],
        out_specs=pl.BlockSpec((rows, d), lambda s: (0, 0)),
        out_shape=jax.ShapeDtypeStruct((rows, d), BF16),
        scratch_shapes=[pltpu.VMEM((rows, d), BF16), pltpu.VMEM((rows, d), BF16), pltpu.VMEM((rows, d), F32)],
        compiler_params=pltpu.CompilerParams(vmem_limit_bytes=60 * 2**20),
        cost_estimate=pl.CostEstimate(flops=2 * rows * d * (d + 2 * f), bytes_accessed=2 * d * (d + 2 * f), transcendentals=0),
        name="mlp",
    )(o, x, g, wo, wu, wd)


def mlp_only_kernel(nf, tm, h_ref, g_ref, wu, wd, y_ref, r_ref, acc_ref):
    s = pl.program_id(0)
    rows, d = h_ref.shape

    @pl.when(s == 0)
    def _():
        def nb(r):
            h = h_ref[pl.ds(r, 128), :]
            r_ref[pl.ds(r, 128), :] = norm_rows(h, g_ref[0])
            acc_ref[pl.ds(r, 128), :] = h.astype(F32)
        row_loop(rows, 128, nb)

    def mb(r):
        z = jnp.dot(r_ref[pl.ds(r, tm), :], wu[0], preferred_element_type=F32)
        z = gelu(z).astype(BF16)
        acc_ref[pl.ds(r, tm), :] += jnp.dot(z, wd[0], preferred_element_type=F32)
    row_loop(rows, tm, mb)

    @pl.when(s == nf - 1)
    def _():
        def nb(r):
            y_ref[pl.ds(r, 128), :] = acc_ref[pl.ds(r, 128), :].astype(BF16)
        row_loop(rows, 128, nb)


def mlp_only_call(h, g, wu, wd, layer, tf=512, tm=512):
    rows, d = h.shape
    f = wu.shape[2]
    nf = f // tf
    return pl.pallas_call(
        functools.partial(mlp_only_kernel, nf, tm),
        grid=(nf,),
        in_specs=[pl.BlockSpec((rows, d), lambda s: (0, 0)), pl.BlockSpec((1, 1, d), lambda s: (layer, 0, 0)),
                  pl.BlockSpec((1, d, tf), lambda s: (layer, 0, s)),
                  pl.BlockSpec((1, tf, d), lambda s: (layer, s, 0))],
        out_specs=pl.BlockSpec((rows, d), lambda s: (0, 0)),
        out_shape=jax.ShapeDtypeStruct((rows, d), BF16),
        scratch_shapes=[pltpu.VMEM((rows, d), BF16), pltpu.VMEM((rows, d), F32)],
        compiler_params=pltpu.CompilerParams(vmem_limit_bytes=48 * 2**20),
        cost_estimate=pl.CostEstimate(flops=4 * rows * d * f, bytes_accessed=4 * d * f, transcendentals=0),
        name="mlp_only",
    )(h, g, wu, wd)


def out_kernel(o_ref, x_ref, wo, h_ref):
    u = jnp.dot(o_ref[...], wo[0], preferred_element_type=F32)
    h_ref[...] = (x_ref[...].astype(F32) + u).astype(BF16)


def out_call(o, x, wo, layer, tn=512):
    rows, d = x.shape
    return pl.pallas_call(
        out_kernel,
        grid=(d // tn,),
        in_specs=[pl.BlockSpec(o.shape, lambda s: (0, 0)), pl.BlockSpec((rows, tn), lambda s: (0, s)),
                  pl.BlockSpec((1, wo.shape[1], tn), lambda s: (layer, 0, s))],
        out_specs=pl.BlockSpec((rows, tn), lambda s: (0, s)),
        out_shape=jax.ShapeDtypeStruct((rows, d), BF16),
        cost_estimate=pl.CostEstimate(flops=2 * rows * d * wo.shape[1], bytes_accessed=2 * d * d, transcendentals=0),
        name="out",
    )(o, x, wo)


def relayout_kernel(wq, wk, wv, oq, ok, ov):
    _, tk, nh, dh = wq.shape
    for w, o in ((wq, oq), (wk, ok), (wv, ov)):
        o[0] = w[0].reshape(tk, nh * dh)


def relayout_call(wq, wk, wv, tk=128):
    nl, d, nh, dh = wq.shape
    ispec = pl.BlockSpec((1, tk, nh, dh), lambda l, s: (l, s, 0, 0))
    ospec = pl.BlockSpec((1, tk, nh * dh), lambda l, s: (l, s, 0))
    out = jax.ShapeDtypeStruct((nl, d, nh * dh), BF16)
    return pl.pallas_call(
        relayout_kernel,
        grid=(nl, d // tk),
        in_specs=[ispec] * 3,
        out_specs=[ospec] * 3,
        out_shape=[out] * 3,
        cost_estimate=pl.CostEstimate(flops=6 * 10**10, bytes_accessed=12 * nl * d * nh * dh, transcendentals=0),
        name="relayout",
    )(wq, wk, wv)


ROPE_BASE = 10000.0


def rope_tables(positions, head_dim):
    inv_freq = ROPE_BASE ** (-jnp.arange(head_dim // 2, dtype=F32) * (2.0 / head_dim))
    angles = positions.astype(F32)[:, None] * inv_freq
    c, s = jnp.cos(angles), jnp.sin(angles)
    return jnp.concatenate([c, c], axis=1), jnp.concatenate([-s, s], axis=1)


def solution(mesh):
    tok_spec = P(None, ("data", "seq"), None)
    in_specs = (tok_spec, P(("data", "seq"))) + (P(),) * 8
    n_dev = mesh.shape["seq"]

    def device_fn(x_loc, pos_loc, w_query, w_key, w_value, w_out, w_up, w_down, g_attn, g_mlp):
        n_seq, shard, d = x_loc.shape
        n_layers, _, n_heads, dh = w_query.shape
        hd = n_heads * dh
        a2a = lambda a: lax.all_to_all(a, "seq", 0, 0, tiled=True)
        pos = lax.all_gather(pos_loc, "seq", tiled=True)
        pos, x_loc = lax.optimization_barrier((pos, x_loc))
        x = a2a(x_loc).reshape(n_dev * shard, d)
        cos, sin = rope_tables(pos, dh)
        wq, wk, wv = relayout_call(w_query, w_key, w_value)
        wo = w_out.reshape(n_layers, hd, d)
        ga, gm = g_attn[:, None, :], g_mlp[:, None, :]
        half = shard // 2
        for l in range(n_layers):
            q, k, v = qkv_call(x, ga, cos, sin, wq, wk, wv, l, tm=1024)
            o = attn_call(q, k, v, dh, hb=4)
            if l < n_layers - 1:
                x = mlp_call(o, x, gm, wo, w_up, w_down, l, tf=1024, tm=1024)
        l = n_layers - 1
        part = lambda a, i: a.reshape(n_dev, shard, a.shape[1])[:, i * half:(i + 1) * half].reshape(n_dev * half, a.shape[1])
        h_a = out_call(part(o, 0), part(x, 0), wo, l)
        h_a = a2a(h_a.reshape(n_dev, half, d))
        y_b = mlp_call(part(o, 1), part(x, 1), gm, wo, w_up, w_down, l, tf=1024, tm=512)
        y_b = a2a(y_b.reshape(n_dev, half, d))
        y_a = mlp_only_call(h_a.reshape(n_dev * half, d), gm, w_up, w_down, l, tf=1024, tm=512).reshape(n_dev, half, d)
        return jnp.concatenate([y_a, y_b], axis=1)

    return jax.shard_map(device_fn, mesh=mesh, in_specs=in_specs, out_specs=tok_spec, check_vma=False)
```

```python
import functools
import jax
import jax.numpy as jnp
from jax import lax
from jax.experimental import pallas as pl
from jax.experimental.pallas import tpu as pltpu
from jax.sharding import PartitionSpec as P

EPS = 1e-6
F32 = jnp.float32
BF16 = jnp.bfloat16


def norm_rows(x, g):
    x = x.astype(F32)
    return (x * lax.rsqrt(jnp.mean(x * x, axis=-1, keepdims=True) + EPS) * g).astype(BF16)


def gelu(x):
    h = 0.5 * x
    return h * jnp.tanh(x * (0.7978845608028654 + 0.035677408136300125 * (x * x))) + h


def row_loop(rows, tile, body):
    if rows == tile:
        body(0)
        return
    def step(i, c):
        body(pl.multiple_of(i * tile, tile))
        return c
    lax.fori_loop(0, rows // tile, step, 0)


def attention(dh, tq, q_ref, k_ref, v_ref, o_ref):
    rows, width = q_ref.shape
    scale = dh ** -0.5 * 1.4426950408889634
    keep = lax.broadcasted_iota(jnp.int32, (tq, tq), 1) <= lax.broadcasted_iota(jnp.int32, (tq, tq), 0)
    jobs = [(slice(h * dh, (h + 1) * dh), i) for h in range(width // dh) for i in range(rows // tq)]

    def score(cs, i):
        n = (i + 1) * tq
        return lax.dot_general(q_ref[i * tq:n, cs], k_ref[:n, cs], (((1,), (1,)), ((), ())), preferred_element_type=F32)

    nxt = score(*jobs[0])
    for j, (cs, i) in enumerate(jobs):
        s = nxt
        if j + 1 < len(jobs):
            nxt = score(*jobs[j + 1])
        n = (i + 1) * tq
        sd = jnp.where(keep, s[:, n - tq:], -1e30)
        s = jnp.concatenate([s[:, :n - tq], sd], axis=1) if i else sd
        m = jnp.max(s, axis=1, keepdims=True)
        e = jnp.exp2((s - m) * scale)
        l = jnp.sum(e, axis=1, keepdims=True)
        o = jnp.dot(e.astype(BF16), v_ref[:n, cs], preferred_element_type=F32)
        o_ref[i * tq:n, cs] = (o / l).astype(BF16)


def layers_kernel(cfg, x_ref, ga_ref, gm_ref, tab_ref, wqkv, wo, wu, wd, ha_ref, hb_ref, n_ref, qkv_ref, acc_ref):
    nx, nq, na, no, nf, last, tq, to, tm = cfg
    t = pl.program_id(0) - nx
    per = nq + na + no + nf
    layer = jnp.maximum(t, 0) // per
    p = lax.rem(jnp.maximum(t, 0), per)
    dh = tab_ref.shape[2]
    ng, rows, gw = qkv_ref.shape
    d = acc_ref.shape[1]

    @pl.when(t < 0)
    def _():
        xr = x_ref.shape[0]
        base = (t + nx) * xr
        def nb(r):
            x = x_ref[pl.ds(r, 128), :]
            rs = pl.ds(pl.multiple_of(base + r, 128), 128)
            n_ref[rs, :] = norm_rows(x, ga_ref[0])
            acc_ref[rs, :] = x.astype(F32)
        row_loop(xr, 128, nb)

    @pl.when((t >= 0) & (p < nq))
    def _():
        tn = wqkv.shape[2]
        k = tn // gw
        tab = jnp.where(p * k < 2 * ng // 3, 0, 1)
        for r in range(0, rows, tq):
            u = jnp.dot(n_ref[r:r + tq, :], wqkv[0], preferred_element_type=F32)
            cs = tab_ref[tab, r:r + tq, :]
            sc = pltpu.roll(cs, dh // 2, 1)
            lo = lax.broadcasted_iota(jnp.int32, cs.shape, 1) < dh // 2
            c = jnp.where(lo, cs, sc)
            sn = jnp.where(lo, -sc, cs)
            for h in range(tn // dh):
                uh = u[:, h * dh:(h + 1) * dh]
                g, o = divmod(h * dh, gw)
                qkv_ref[p * k + g, r:r + tq, o:o + dh] = (uh * c + pltpu.roll(uh, dh // 2, 1) * sn).astype(BF16)

    @pl.when((p >= nq) & (p < nq + na))
    def _():
        a = p - nq
        attention(dh, 256, qkv_ref.at[a], qkv_ref.at[na + a], qkv_ref.at[2 * na + a], qkv_ref.at[a])

    @pl.when((p >= nq + na) & (p < nq + na + no))
    def _():
        tn = wo.shape[2]
        half = ha_ref.shape[1]
        nd = to // (2 * half)
        cs = pl.ds(pl.multiple_of((p - nq - na) * tn, tn), tn)
        for r in range(0, rows, to):
            o = jnp.concatenate([qkv_ref[a, r:r + to, :] for a in range(na)], axis=1)
            u = jnp.dot(o, wo[0], preferred_element_type=F32)
            h = (acc_ref[r:r + to, cs] + u).astype(BF16)
            acc_ref[r:r + to, cs] = h.astype(F32)
            h = h.reshape(nd, 2 * half, tn)
            i = r // (2 * half)
            ha_ref[i:i + nd] = h[:, :half]
            hb_ref[i:i + nd] = h[:, half:]

    @pl.when(p == nq + na + no)
    def _():
        def nb(r):
            n_ref[pl.ds(r, 128), :] = norm_rows(acc_ref[pl.ds(r, 128), :], gm_ref[0])
        row_loop(rows, 128, nb)

    @pl.when(p >= nq + na + no)
    def _():
        for r in range(0, rows, tm):
            z = jnp.dot(n_ref[r:r + tm, :], wu[0], preferred_element_type=F32)
            z = gelu(z).astype(BF16)
            acc_ref[r:r + tm, :] += jnp.dot(z, wd[0], preferred_element_type=F32)

    @pl.when(p == per - 1)
    def _():
        def nb(r):
            y = acc_ref[pl.ds(r, 128), :].astype(BF16)
            acc_ref[pl.ds(r, 128), :] = y.astype(F32)
            n_ref[pl.ds(r, 128), :] = norm_rows(y, ga_ref[0])
        row_loop(rows, 128, nb)


def layers_call(x, ga, gm, table, wqkv, wo, wu, wd, n_dev, tnq=1024, tno=512, tf=1024, gw=512, xr=128, tq=256, to=256, tm=1024):
    rows, d = x.shape
    nl, _, hd3 = wqkv.shape
    hd = hd3 // 3
    f = wu.shape[2]
    half = rows // n_dev // 2
    nx, nq, na, no, nf, last = rows // xr, hd3 // tnq, hd // gw, d // tno, f // tf, nl - 1
    per = nq + na + no + nf
    grid = nx + last * per + nq + na + no

    def lp(s):
        t = jnp.maximum(s - nx, 0)
        return t // per, lax.rem(t, per)

    def gain_map(s):
        l, p = lp(s)
        return jnp.minimum(l + jnp.where(p == per - 1, 1, 0), last), 0, 0

    def qkv_map(s):
        l, p = lp(s)
        return l, 0, jnp.minimum(p, nq - 1)

    def out_map(s):
        l, p = lp(s)
        return l, 0, jnp.clip(p - nq - na, 0, no - 1)

    def ff_map(s):
        l, p = lp(s)
        return jnp.minimum(l, last - 1), jnp.where(l == last, nf - 1, jnp.clip(p - nq - na - no, 0, nf - 1))

    def up_map(s):
        l, c = ff_map(s)
        return l, 0, c

    def down_map(s):
        l, c = ff_map(s)
        return l, c, 0

    def h_map(s):
        l, p = lp(s)
        return 0, 0, jnp.where(l == last, jnp.clip(p - nq - na, 0, no - 1), 0)

    once = pl.Buffered(1)
    tab = pl.BlockSpec(table.shape, lambda s: (0, 0, 0), pipeline_mode=once)
    out = jax.ShapeDtypeStruct((n_dev, half, d), BF16)
    return pl.pallas_call(
        functools.partial(layers_kernel, (nx, nq, na, no, nf, last, tq, to, tm)),
        grid=(grid,),
        in_specs=[pl.BlockSpec((xr, d), lambda s: (jnp.minimum(s, nx - 1), 0)),
                  pl.BlockSpec((1, 1, d), gain_map), pl.BlockSpec((1, 1, d), lambda s: (lp(s)[0], 0, 0)), tab,
                  pl.BlockSpec((1, d, tnq), qkv_map), pl.BlockSpec((1, hd, tno), out_map),
                  pl.BlockSpec((1, d, tf), up_map), pl.BlockSpec((1, tf, d), down_map)],
        out_specs=[pl.BlockSpec((n_dev, half, tno), h_map)] * 2,
        out_shape=[out, out],
        scratch_shapes=[pltpu.VMEM((rows, d), BF16), pltpu.VMEM((3 * na, rows, gw), BF16), pltpu.VMEM((rows, d), F32)],
        compiler_params=pltpu.CompilerParams(vmem_limit_bytes=67043328),
        cost_estimate=pl.CostEstimate(flops=2 * rows * (nl * d * 4 * hd + 2 * last * d * f), bytes_accessed=2 * (nl * d * 4 * hd + 2 * last * d * f), transcendentals=0),
        name="layers",
    )(x, ga, gm, table, wqkv, wo, wu, wd)


def mlp_only_kernel(nf, tm, h_ref, g_ref, wu, wd, y_ref, r_ref, acc_ref):
    s = pl.program_id(0)
    rows, d = h_ref.shape

    @pl.when(s == 0)
    def _():
        def nb(r):
            h = h_ref[pl.ds(r, 128), :]
            r_ref[pl.ds(r, 128), :] = norm_rows(h, g_ref[0])
            acc_ref[pl.ds(r, 128), :] = h.astype(F32)
        row_loop(rows, 128, nb)

    def mb(r):
        z = jnp.dot(r_ref[pl.ds(r, tm), :], wu[0], preferred_element_type=F32)
        z = gelu(z).astype(BF16)
        acc_ref[pl.ds(r, tm), :] += jnp.dot(z, wd[0], preferred_element_type=F32)
    row_loop(rows, tm, mb)

    @pl.when(s == nf - 1)
    def _():
        def nb(r):
            y_ref[pl.ds(r, 128), :] = acc_ref[pl.ds(r, 128), :].astype(BF16)
        row_loop(rows, 128, nb)


def mlp_only_call(h, g, wu, wd, layer, tf=512, tm=512):
    rows, d = h.shape
    f = wu.shape[2]
    nf = f // tf
    return pl.pallas_call(
        functools.partial(mlp_only_kernel, nf, tm),
        grid=(nf,),
        in_specs=[pl.BlockSpec((rows, d), lambda s: (0, 0)), pl.BlockSpec((1, 1, d), lambda s: (layer, 0, 0)),
                  pl.BlockSpec((1, d, tf), lambda s: (layer, 0, s)),
                  pl.BlockSpec((1, tf, d), lambda s: (layer, s, 0))],
        out_specs=pl.BlockSpec((rows, d), lambda s: (0, 0)),
        out_shape=jax.ShapeDtypeStruct((rows, d), BF16),
        scratch_shapes=[pltpu.VMEM((rows, d), BF16), pltpu.VMEM((rows, d), F32)],
        compiler_params=pltpu.CompilerParams(vmem_limit_bytes=60 * 2**20),
        cost_estimate=pl.CostEstimate(flops=4 * rows * d * f, bytes_accessed=4 * d * f, transcendentals=0),
        name="mlp_only",
    )(h, g, wu, wd)


def relayout_kernel(wq, wk, wv, o_ref):
    _, tk, nh, dh = wq.shape
    hd = nh * dh
    for i, w in enumerate((wq, wk, wv)):
        o_ref[0, :, i * hd:(i + 1) * hd] = w[0].reshape(tk, hd)


def relayout_call(wq, wk, wv, tk=128):
    nl, d, nh, dh = wq.shape
    return pl.pallas_call(
        relayout_kernel,
        grid=(nl, d // tk),
        in_specs=[pl.BlockSpec((1, tk, nh, dh), lambda l, s: (l, s, 0, 0))] * 3,
        out_specs=pl.BlockSpec((1, tk, 3 * nh * dh), lambda l, s: (l, s, 0)),
        out_shape=jax.ShapeDtypeStruct((nl, d, 3 * nh * dh), BF16),
        cost_estimate=pl.CostEstimate(flops=6 * 10**10, bytes_accessed=12 * nl * d * nh * dh, transcendentals=0),
        name="relayout",
    )(wq, wk, wv)


ROPE_BASE = 10000.0


def rope_tables(positions, head_dim):
    inv_freq = ROPE_BASE ** (-jnp.arange(head_dim // 2, dtype=F32) * (2.0 / head_dim))
    angles = positions.astype(F32)[:, None] * inv_freq
    c, s = jnp.cos(angles), jnp.sin(angles)
    one, zero = jnp.ones_like(c), jnp.zeros_like(s)
    return jnp.stack([jnp.concatenate([c, s], axis=1), jnp.concatenate([one, zero], axis=1)])


def solution(mesh):
    tok_spec = P(None, ("data", "seq"), None)
    in_specs = (tok_spec, P(("data", "seq"))) + (P(),) * 8
    n_dev = mesh.shape["seq"]

    def device_fn(x_loc, pos_loc, w_query, w_key, w_value, w_out, w_up, w_down, g_attn, g_mlp):
        n_seq, shard, d = x_loc.shape
        n_layers, _, n_heads, dh = w_query.shape
        hd = n_heads * dh
        a2a = lambda a: lax.all_to_all(a, "seq", 0, 0, tiled=True)
        pos = a2a(jnp.broadcast_to(pos_loc[None], (n_dev, shard))).reshape(n_dev * shard)
        x = a2a(x_loc).reshape(n_dev * shard, d)
        table = rope_tables(pos, dh)
        wqkv = relayout_call(w_query, w_key, w_value)
        wo = w_out.reshape(n_layers, hd, d)
        ga, gm = g_attn[:, None, :], g_mlp[:, None, :]
        half = shard // 2
        last = n_layers - 1

        h_a, h_b = layers_call(x, ga, gm, table, wqkv, wo, w_up, w_down, n_dev)
        mlp = lambda h: mlp_only_call(h.reshape(n_dev * half, d), gm, w_up, w_down, last, tf=1024, tm=512).reshape(n_dev, half, d)
        h_a = a2a(h_a)
        y_b = a2a(mlp(h_b))
        y_a = mlp(h_a)
        return jnp.concatenate([y_a, y_b], axis=1)

    return jax.shard_map(device_fn, mesh=mesh, in_specs=in_specs, out_specs=tok_spec, check_vma=False)
```
